128 devices in a mesh: rep: 1, r: 4 (over x), s: 32 (over y, z, core).
Axes of the slice: x: 4, y: 4, z: 4, core: 2. Of those that a mesh axis runs over, the one named last changes fastest.
Arguments:
- x: bfloat16 [128, 2048, 1152], P(('rep', 'r', 's'))
- dy: bfloat16 [128, 2048, 1152], P(('rep', 'r', 's'))
- w_gate: bfloat16 [2, 1152, 4608], P(None, 's')
- w_up: bfloat16 [2, 1152, 4608], P(None, 's')
- w_down: bfloat16 [2, 4608, 1152], P(None, 's')
Outputs:
- output 1: bfloat16 [128, 2048, 1152], P(('rep', 'r', 's'))
- output 2: bfloat16 [2, 1152, 4608], P('rep', 's')
- output 3: bfloat16 [2, 1152, 4608], P('rep', 's')
- output 4: bfloat16 [2, 4608, 1152], P('rep', 's')
All inputs are finite; a program needn't handle non-finite values.
Results may differ from the reference program's by a relative error of at most 0.018.
Values are sent between devices in bfloat16 or wider.
A program may use at most 1.5 GiB of HBM per device.

```python
import jax
import jax.numpy as jnp
from jax import lax

SEQUENCES = 128
TOKENS = 2048
D = 1152
FF = 4608
LAYERS = 2
NAMES = ("w_gate", "w_up", "w_down")
SHAPES = {"w_gate": (LAYERS, D, FF), "w_up": (LAYERS, D, FF), "w_down": (LAYERS, FF, D)}


def bump(key, n, height):
    away = (jnp.arange(n, dtype=jnp.int32) - jax.random.randint(key, (), 0, n, jnp.int32)) % n
    return jnp.where(away < n // 8, height, 1.0)


def together(key, own, strength):
    shared = jax.random.normal(key, own.shape[1:], jnp.float32)
    return (own + strength * shared) * lax.rsqrt(1 + strength * strength)


def setup_inputs(seed: int = 0, part: int = 0) -> dict:
    kx, kdy, ka, kb, kz, kf, kh, kl, *kw = jax.random.split(jax.random.key(seed), 8 + len(NAMES))
    kx, kdy, ka, kb = (jax.random.fold_in(k, part) for k in (kx, kdy, ka, kb))
    shape = (SEQUENCES, TOKENS, D)
    much_x, much_dy = jax.random.uniform(kz, (2,), jnp.float32, 0.0, 1.0)
    layers = 2.0 ** jax.random.uniform(kl, (LAYERS, 1, 1), jnp.float32, -1.0, 1.0)
    x = together(ka, jax.random.normal(kx, shape, jnp.float32), much_x) * bump(kf, D, 4.0)
    dy = together(kb, jax.random.normal(kdy, shape, jnp.float32), much_dy)
    drawn = {"x": x.astype(jnp.bfloat16), "dy": (dy * (SEQUENCES * TOKENS) ** -0.5).astype(jnp.bfloat16)}
    for key, name in zip(kw, NAMES, strict=True):
        w = jax.random.normal(key, SHAPES[name], jnp.float32) * SHAPES[name][1] ** -0.5
        drawn[name] = (w * {"w_gate": 1.0, "w_up": bump(kh, FF, 4.0), "w_down": layers}[name]).astype(jnp.bfloat16)
    return drawn


def matmul(a, w):
    return jnp.dot(a, w, preferred_element_type=jnp.float32).astype(jnp.bfloat16)


def normed(h):
    wide = h.astype(jnp.float32)
    scale = lax.rsqrt(jnp.mean(wide**2, -1, keepdims=True) + 1e-6)
    return (wide * scale).astype(jnp.bfloat16)


def layer(h, w):
    a = normed(h)
    gate = jnp.dot(a, w["w_gate"], preferred_element_type=jnp.float32)
    up = jnp.dot(a, w["w_up"], preferred_element_type=jnp.float32)
    return h + matmul((jax.nn.silu(gate) * up).astype(jnp.bfloat16), w["w_down"])


def stack(weights, h):
    return lax.scan(lambda h, w: (layer(h, w), None), h, weights)[0]


def reference(x, dy, w_gate, w_up, w_down):
    weights = dict(zip(NAMES, (w_gate, w_up, w_down), strict=True))

    def take(so_far, sequence):
        h, by_y = sequence
        _, back = jax.vjp(stack, weights, h)
        by_weights, by_h = back(by_y)
        return jax.tree.map(lambda total, term: total + term.astype(jnp.float32), so_far, by_weights), by_h

    none_yet = {name: jnp.zeros(w.shape, jnp.float32) for name, w in weights.items()}
    by_weights, by_x = lax.scan(take, none_yet, (x, dy))
    return (by_x, *(by_weights[name].astype(jnp.bfloat16) for name in NAMES))
```

```python
import jax
import jax.numpy as jnp
from jax import lax
from jax.experimental import pallas as pl
from jax.experimental.pallas import tpu as pltpu
from jax.sharding import Mesh, PartitionSpec as P

F32, BF16 = jnp.float32, jnp.bfloat16
PLANE = ("y", "z", "c")
FF_BLOCK = 512
FF_PART = 256
ROWS = 512
PARAMS = dict(vmem_limit_bytes=62 * 1024 * 1024)


def dot(a, b, dims=((1,), (0,)), out=F32):
    return lax.dot_general(a, b, (dims, ((), ())), preferred_element_type=F32).astype(out)


def inner_loop(tokens, body):
    @pl.loop(0, tokens // ROWS)
    def _(i):
        body(pl.ds(pl.multiple_of(i * ROWS, ROWS), ROWS))


def columns():
    for start in range(0, FF_BLOCK, FF_PART):
        yield pl.ds(start, FF_PART), pl.ds(FF_BLOCK + start, FF_PART)


def forward_kernel(a, w, gate, up, act):
    def body(rows):
        for c, above in columns():
            g, u = dot(a[rows, :], w[:, c]), dot(a[rows, :], w[:, above])
            gate[rows, c], up[rows, c] = g, u
            act[rows, c] = (g * lax.logistic(g) * u).astype(BF16)

    inner_loop(a.shape[0], body)


def projections_gradient(by, g, u, s):
    return (by * u * (s + g * s * (1 - s))).astype(BF16), (by * (g * s)).astype(BF16)


def last_kernel(a, w, by_out, w_down, act, by_proj):
    def body(rows):
        for c, above in columns():
            g, u = dot(a[rows, :], w[:, c]), dot(a[rows, :], w[:, above])
            by = dot(by_out[rows, :], w_down[c, :], ((1,), (1,)), BF16).astype(F32)
            s = lax.logistic(g)
            act[rows, c] = (g * s * u).astype(BF16)
            by_proj[rows, c], by_proj[rows, above] = projections_gradient(by, g, u, s)

    inner_loop(a.shape[0], body)


def backward_kernel(by_out, w_down, gate, up, by_proj):
    def body(rows):
        for c, above in columns():
            by = dot(by_out[rows, :], w_down[c, :], ((1,), (1,)), BF16).astype(F32)
            g = gate[rows, c]
            by_proj[rows, c], by_proj[rows, above] = projections_gradient(by, g, up[rows, c], lax.logistic(g))

    inner_loop(by_out.shape[0], body)


def solution(mesh):
    finer = Mesh(mesh.devices.reshape(mesh.shape["rep"], mesh.shape["r"], 4, 4, 2), ("rep", "r", "y", "z", "c"))

    def step(x, dy, w_gate, w_up, w_down):
        layers, share, ff = w_gate.shape
        tokens, d = x.shape[1:]
        devices = 32
        part = -(-share // 8) * 8
        wide = devices * part
        blocks = ff // FF_BLOCK
        full = lambda shape: pl.BlockSpec(shape, lambda *_: (0, 0))

        spread_to = jnp.arange(d) // share * part + jnp.arange(d) % share
        spread = (spread_to[:, None] == jnp.arange(wide)[None, :]).astype(BF16)
        core = lax.axis_index("c")
        half = wide // 2
        taken = jnp.arange(half) // part * 2 * part + jnp.arange(half) % part

        def rows_of(core):
            return (jnp.arange(wide)[:, None] == (taken + core * part)[None, :]).astype(BF16)

        def normed(h):
            w = h.astype(F32)
            return (w * lax.rsqrt(jnp.sum(w**2, -1, keepdims=True) / d + 1e-6)).astype(BF16)

        def gathered(block):
            return lax.all_gather(block, PLANE, axis=0, tiled=True)

        def gate_up(n):
            fill = lambda w: jnp.pad(w[n], ((0, part - share), (0, 0)))
            mixed = jnp.stack([fill(w).reshape(part, blocks, FF_BLOCK) for w in (w_gate, w_up)], 2)
            return gathered(mixed.reshape(part, 2 * ff))

        def apart(mixed):
            return tuple(mixed.reshape(part, blocks, 2, FF_BLOCK)[:share, :, i].reshape(share, ff) for i in range(2))

        gu0 = gate_up(0)
        downs = gathered(jnp.concatenate([dot(w_down[n], spread, out=BF16) for n in range(2)], 1))
        gu1 = gate_up(1)
        h0, by_y = dot(x[0], spread, out=BF16), dot(dy[0], spread, out=BF16)

        a0 = normed(h0)
        pair = pl.BlockSpec((wide, 2 * FF_BLOCK), lambda j: (0, j))
        cols = pl.BlockSpec((tokens, FF_BLOCK), lambda j: (0, j))
        kept = jax.ShapeDtypeStruct((tokens, ff), F32)
        rounded = jax.ShapeDtypeStruct((tokens, ff), BF16)
        flops = 2 * tokens * d * ff
        gate0, up0, act0 = pl.pallas_call(
            forward_kernel, grid=(blocks,), in_specs=[full((tokens, wide)), pair], out_specs=[cols] * 3,
            out_shape=[kept, kept, rounded], compiler_params=pltpu.CompilerParams(**PARAMS), name="forward_0",
            cost_estimate=pl.CostEstimate(flops=2 * flops, bytes_accessed=tokens * ff * 10 + 2 * wide * ff * 2, transcendentals=0),
        )(a0, gu0)
        down0 = downs[:, :wide]
        h1 = h0 + dot(act0, down0, out=BF16)
        from_other, from_mine = dot(a0, rows_of(1 - core), out=BF16), dot(a0, rows_of(core), out=BF16)
        a1, from_other, from_mine = lax.optimization_barrier((normed(h1), from_other, from_mine))

        down = lambda n: pl.BlockSpec((FF_BLOCK, wide), lambda j: (j, n))
        pairs = pl.BlockSpec((tokens, 2 * FF_BLOCK), lambda j: (0, j))
        both = jax.ShapeDtypeStruct((tokens, 2 * ff), BF16)
        act1, by_gu1 = pl.pallas_call(
            last_kernel, grid=(blocks,), in_specs=[full((tokens, wide)), pair, full((tokens, wide)), down(1)],
            out_specs=[cols, pairs], out_shape=[rounded, both],
            compiler_params=pltpu.CompilerParams(**PARAMS), name="last_1",
            cost_estimate=pl.CostEstimate(flops=3 * flops, bytes_accessed=tokens * ff * 6 + 3 * wide * ff * 2, transcendentals=0),
        )(a1, gu1, by_y, downs)
        scattered = lambda term: lax.psum_scatter(term, PLANE, scatter_dimension=0, tiled=True)
        over_tokens = ((0,), (0,))
        w1 = dot(a1, by_gu1, over_tokens, BF16)
        act1, by_gu1, w1 = lax.optimization_barrier((act1, by_gu1, w1))
        w1 = scattered(w1)
        d1 = dot(act1, by_y, over_tokens, BF16)
        by_gu1, d1 = lax.optimization_barrier((by_gu1, d1))
        d1 = scattered(d1)

        def through_norm(h, by_a, by_h):
            return by_h + jax.vjp(normed, h)[1](by_a)[0]

        by_h = through_norm(h1, dot(by_gu1, gu1, ((1,), (1,)), BF16), by_y)

        d0 = dot(act0, by_h, over_tokens, BF16)
        by_h, d0 = lax.optimization_barrier((by_h, d0))
        d0 = scattered(d0)
        by_gu0 = pl.pallas_call(
            backward_kernel, grid=(blocks,), in_specs=[full((tokens, wide)), down(0), cols, cols],
            out_specs=pairs, out_shape=both,
            compiler_params=pltpu.CompilerParams(**PARAMS), name="backward_0",
            cost_estimate=pl.CostEstimate(flops=flops, bytes_accessed=tokens * ff * 12 + wide * ff * 2, transcendentals=0),
        )(by_h, downs, gate0, up0)

        half_of = lambda w, i: w[:, i * ff:(i + 1) * ff]
        theirs, mine = [], []
        for i in range(2):
            other = dot(from_other, half_of(by_gu0, i), over_tokens, BF16)
            by_gu0, other = lax.optimization_barrier((by_gu0, other))
            theirs.append(lax.ppermute(other, "c", [(0, 1), (1, 0)]))
        for i in range(2):
            total = dot(from_mine, half_of(by_gu0, i), over_tokens) + theirs[i].astype(F32)
            by_gu0, total = lax.optimization_barrier((by_gu0, total))
            mine.append(total)

        def along(axis, dim, term):
            me = lax.axis_index(axis)
            piece = lambda k: lax.dynamic_index_in_dim(term, (me + k) % 4, dim, keepdims=False)
            came = [lax.ppermute(piece(k).astype(BF16), axis, [(i, (i + k) % 4) for i in range(4)]) for k in (1, 3, 2)]
            return piece(0) + came[0].astype(F32) + came[1].astype(F32) + came[2].astype(F32)

        def copies(term):
            t = term.astype(BF16)
            came = [lax.ppermute(t, "r", [(i, i ^ k) for i in range(4)]).astype(F32) for k in (1, 2, 3)]
            return ((t.astype(F32) + came[0]) + (came[1] + came[2])).astype(BF16)

        view = (4, 4, part, ff)
        by_a = dot(half_of(by_gu0, 0), half_of(gu0, 0), ((1,), (1,)))
        sums = along("y", 0, mine[0].reshape(view)), along("z", 1, mine[1].reshape(view))
        by_gu0, by_a, sums = lax.optimization_barrier((by_gu0, by_a, sums))
        by_a = (by_a + dot(half_of(by_gu0, 1), half_of(gu0, 1), ((1,), (1,)))).astype(BF16)
        sums = along("z", 0, sums[0]), along("y", 0, sums[1])
        by_a, sums, d1, w1, d0 = lax.optimization_barrier((by_a, sums, d1, w1, d0))
        w0 = jnp.concatenate([copies(t) for t in sums], 1)
        by_x = dot(through_norm(h0, by_a, by_h), spread, ((1,), (1,)), BF16)
        d1, w1, d0 = lax.psum((d1, w1, d0), "r")
        narrow = lambda w: dot(w, spread, ((1,), (1,)), BF16)
        return (
            by_x[None],
            *(jnp.stack(w) for w in zip(apart(w0), apart(w1))),
            jnp.stack([narrow(d0), narrow(d1)]),
        )

    states, cut = P(("rep", "r", *PLANE), None, None), P(None, PLANE, None)
    return jax.shard_map(
        step,
        mesh=finer,
        in_specs=(states, states) + (cut,) * 3,
        out_specs=(states,) + (P("rep", PLANE, None),) * 3,
        check_vma=False,
    )
```

```python
import jax
import jax.numpy as jnp
from jax import lax
from jax.experimental import pallas as pl
from jax.experimental.pallas import tpu as pltpu
from jax.sharding import Mesh, PartitionSpec as P

F32, BF16 = jnp.float32, jnp.bfloat16
PLANE = ("y", "z", "c")
FF_BLOCK = 512
FF_PART = 256
ROWS = 512
PARAMS = dict(vmem_limit_bytes=62 * 1024 * 1024)


def dot(a, b, dims=((1,), (0,)), out=F32):
    return lax.dot_general(a, b, (dims, ((), ())), preferred_element_type=F32).astype(out)


def inner_loop(tokens, body):
    @pl.loop(0, tokens // ROWS)
    def _(i):
        body(pl.ds(pl.multiple_of(i * ROWS, ROWS), ROWS))


def columns():
    for start in range(0, FF_BLOCK, FF_PART):
        yield pl.ds(start, FF_PART), pl.ds(FF_BLOCK + start, FF_PART)


def forward_kernel(a, w, gate, up, act):
    def body(rows):
        for c, above in columns():
            g, u = dot(a[rows, :], w[:, c]), dot(a[rows, :], w[:, above])
            gate[rows, c], up[rows, c] = g, u
            act[rows, c] = (g * lax.logistic(g) * u).astype(BF16)

    inner_loop(a.shape[0], body)


def projections_gradient(by, g, u, s):
    return (by * u * (s + g * s * (1 - s))).astype(BF16), (by * (g * s)).astype(BF16)


def last_kernel(a, w, by_act, act, by_proj):
    def body(rows):
        for c, above in columns():
            g, u = dot(a[rows, :], w[:, c]), dot(a[rows, :], w[:, above])
            by = by_act[rows, c].astype(F32)
            s = lax.logistic(g)
            act[rows, c] = (g * s * u).astype(BF16)
            by_proj[rows, c], by_proj[rows, above] = projections_gradient(by, g, u, s)

    inner_loop(a.shape[0], body)


def backward_kernel(by_out, w_down, gate, up, by_proj):
    def body(rows):
        for c, above in columns():
            by = dot(by_out[rows, :], w_down[c, :], ((1,), (1,)), BF16).astype(F32)
            g = gate[rows, c]
            by_proj[rows, c], by_proj[rows, above] = projections_gradient(by, g, up[rows, c], lax.logistic(g))

    inner_loop(by_out.shape[0], body)


def solution(mesh):
    finer = Mesh(mesh.devices.reshape(mesh.shape["rep"], mesh.shape["r"], 4, 4, 2), ("rep", "r", "y", "z", "c"))

    def step(x, dy, w_gate, w_up, w_down):
        layers, share, ff = w_gate.shape
        tokens, d = x.shape[1:]
        devices = 32
        part = -(-share // 8) * 8
        wide = devices * part
        blocks = ff // FF_BLOCK
        full = lambda shape: pl.BlockSpec(shape, lambda *_: (0, 0))

        spread_to = jnp.arange(d) // share * part + jnp.arange(d) % share
        spread = (spread_to[:, None] == jnp.arange(wide)[None, :]).astype(BF16)
        core = lax.axis_index("c")
        half = wide // 2
        taken = jnp.arange(half) // part * 2 * part + jnp.arange(half) % part

        def rows_of(core):
            return (jnp.arange(wide)[:, None] == (taken + core * part)[None, :]).astype(BF16)

        def normed(h):
            w = h.astype(F32)
            return (w * lax.rsqrt(jnp.sum(w**2, -1, keepdims=True) / d + 1e-6)).astype(BF16)

        def gathered(block):
            return lax.all_gather(block, PLANE, axis=0, tiled=True)

        def gate_up(n):
            fill = lambda w: jnp.pad(w[n], ((0, part - share), (0, 0)))
            mixed = jnp.stack([fill(w).reshape(part, blocks, FF_BLOCK) for w in (w_gate, w_up)], 2)
            return gathered(mixed.reshape(part, 2 * ff))

        def apart(mixed):
            return tuple(mixed.reshape(part, blocks, 2, FF_BLOCK)[:share, :, i].reshape(share, ff) for i in range(2))

        gu0 = gate_up(0)
        downs = gathered(jnp.concatenate([dot(w_down[n], spread, out=BF16) for n in range(2)], 1))
        gu1 = gate_up(1)
        h0, by_y = dot(x[0], spread, out=BF16), dot(dy[0], spread, out=BF16)

        a0 = normed(h0)
        pair = pl.BlockSpec((wide, 2 * FF_BLOCK), lambda j: (0, j))
        cols = pl.BlockSpec((tokens, FF_BLOCK), lambda j: (0, j))
        kept = jax.ShapeDtypeStruct((tokens, ff), F32)
        rounded = jax.ShapeDtypeStruct((tokens, ff), BF16)
        flops = 2 * tokens * d * ff
        gate0, up0, act0 = pl.pallas_call(
            forward_kernel, grid=(blocks,), in_specs=[full((tokens, wide)), pair], out_specs=[cols] * 3,
            out_shape=[kept, kept, rounded], compiler_params=pltpu.CompilerParams(**PARAMS), name="forward_0",
            cost_estimate=pl.CostEstimate(flops=2 * flops, bytes_accessed=tokens * ff * 10 + 2 * wide * ff * 2, transcendentals=0),
        )(a0, gu0)
        down0 = downs[:, :wide]
        h1 = h0 + dot(act0, down0, out=BF16)
        from_other, from_mine = dot(a0, rows_of(1 - core), out=BF16), dot(a0, rows_of(core), out=BF16)
        a1, downs, by_y, from_other, from_mine = lax.optimization_barrier((normed(h1), downs, by_y, from_other, from_mine))
        by_act1 = dot(by_y, downs[:, wide:], ((1,), (1,)), BF16)

        down = lambda n: pl.BlockSpec((FF_BLOCK, wide), lambda j: (j, n))
        pairs = pl.BlockSpec((tokens, 2 * FF_BLOCK), lambda j: (0, j))
        both = jax.ShapeDtypeStruct((tokens, 2 * ff), BF16)
        act1, by_gu1 = pl.pallas_call(
            last_kernel, grid=(blocks,), in_specs=[full((tokens, wide)), pair, cols],
            out_specs=[cols, pairs], out_shape=[rounded, both],
            compiler_params=pltpu.CompilerParams(**PARAMS), name="last_1",
            cost_estimate=pl.CostEstimate(flops=2 * flops, bytes_accessed=tokens * ff * 8 + 2 * wide * ff * 2, transcendentals=0),
        )(a1, gu1, by_act1)
        scattered = lambda term: lax.psum_scatter(term, PLANE, scatter_dimension=0, tiled=True)
        over_tokens = ((0,), (0,))
        w1 = dot(a1, by_gu1, over_tokens, BF16)
        act1, by_gu1, w1 = lax.optimization_barrier((act1, by_gu1, w1))
        w1 = scattered(w1)
        d1 = dot(act1, by_y, over_tokens, BF16)
        by_gu1, d1 = lax.optimization_barrier((by_gu1, d1))

        def through_norm(h, by_a, by_h):
            return by_h + jax.vjp(normed, h)[1](by_a)[0]

        by_h = through_norm(h1, dot(by_gu1, gu1, ((1,), (1,)), BF16), by_y)

        d0 = dot(act0, by_h, over_tokens, BF16)
        by_h, wd = lax.optimization_barrier((by_h, jnp.concatenate([d0, d1], 1)))
        wd = scattered(wd)
        by_gu0 = pl.pallas_call(
            backward_kernel, grid=(blocks,), in_specs=[full((tokens, wide)), down(0), cols, cols],
            out_specs=pairs, out_shape=both,
            compiler_params=pltpu.CompilerParams(**PARAMS), name="backward_0",
            cost_estimate=pl.CostEstimate(flops=flops, bytes_accessed=tokens * ff * 12 + wide * ff * 2, transcendentals=0),
        )(by_h, downs, gate0, up0)

        half_of = lambda w, i: w[:, i * ff:(i + 1) * ff]
        theirs, mine = [], []
        for i in range(2):
            other = dot(from_other, half_of(by_gu0, i), over_tokens, BF16)
            by_gu0, other = lax.optimization_barrier((by_gu0, other))
            theirs.append(lax.ppermute(other, "c", [(0, 1), (1, 0)]))
        for i in range(2):
            total = dot(from_mine, half_of(by_gu0, i), over_tokens) + theirs[i].astype(F32)
            by_gu0, total = lax.optimization_barrier((by_gu0, total))
            mine.append(total)

        def along(axis, dim, term):
            me = lax.axis_index(axis)
            piece = lambda k: lax.dynamic_index_in_dim(term, (me + k) % 4, dim, keepdims=False)
            came = [lax.ppermute(piece(k).astype(BF16), axis, [(i, (i + k) % 4) for i in range(4)]) for k in (1, 3, 2)]
            return piece(0) + came[0].astype(F32) + came[1].astype(F32) + came[2].astype(F32)

        def copies(term):
            t = term.astype(BF16)
            came = [lax.ppermute(t, "r", [(i, i ^ k) for i in range(4)]).astype(F32) for k in (1, 2, 3)]
            return ((t.astype(F32) + came[0]) + (came[1] + came[2])).astype(BF16)

        view = (4, 4, part, ff)
        by_a = [dot(by_gu0[:tokens // 2], gu0, ((1,), (1,)), BF16)]
        sums = along("y", 0, mine[0].reshape(view)), along("z", 1, mine[1].reshape(view))
        by_gu0, by_a, sums = lax.optimization_barrier((by_gu0, by_a, sums))
        by_a = jnp.concatenate(by_a + [dot(by_gu0[tokens // 2:], gu0, ((1,), (1,)), BF16)])
        sums = along("z", 0, sums[0]), along("y", 0, sums[1])
        by_a, sums = lax.optimization_barrier((by_a, sums))
        w0 = jnp.concatenate([copies(t) for t in sums], 1)
        by_x = dot(through_norm(h0, by_a, by_h), spread, ((1,), (1,)), BF16)
        w1, wd = lax.psum((w1, wd), "r")
        narrow = lambda w: dot(w, spread, ((1,), (1,)), BF16)
        return (
            by_x[None],
            *(jnp.stack(w) for w in zip(apart(w0), apart(w1))),
            jnp.stack([narrow(wd[:, :wide]), narrow(wd[:, wide:])]),
        )

    states, cut = P(("rep", "r", *PLANE), None, None), P(None, PLANE, None)
    return jax.shard_map(
        step,
        mesh=finer,
        in_specs=(states, states) + (cut,) * 3,
        out_specs=(states,) + (P("rep", PLANE, None),) * 3,
        check_vma=False,
    )
```
